32 devices in a mesh: head: 8 (over z, y), batch: 4 (over x, core).
Axes of the slice: x: 2, y: 2, z: 4, core: 2. Of those that a mesh axis runs over, the one named last changes fastest.
Arguments:
- incoming_hidden_stream: bfloat16 [512, 4096], P('batch'), may hold values from -6 to 6
- reception_projection: bfloat16 [4096, 4096], P(None, 'head'), may hold values from -0.09375 to 0.09375
- address_projection: bfloat16 [4096, 4096], P(None, 'head'), may hold values from -0.09375 to 0.09375
- payload_projection: bfloat16 [4096, 4096], P(None, 'head'), may hold values from -0.09375 to 0.09375
- sigmoid_filter_matrix: bfloat16 [4096, 4096], P(None, 'head'), may hold values from -0.09375 to 0.09375
- forgetting_speed: float32 [512, 4096], P('batch', 'head'), may hold values from 0.01 to 1.5
- adaptation_step_size: float32 [512, 4096], P('batch', 'head'), may hold values from 0 to 1
- diagonal_boost: float32 [4096], P('head'), may hold values from -0.6 to 0.6
- subspace_standardize_scale: float32 [4096], P('head'), may hold values from 0.5 to 2
- recurrent_memory_matrix: float32 [64, 64, 64, 64], P('batch', 'head'), may hold values from -6 to 6
- emission_projection: bfloat16 [4096, 4096], P('head'), may hold values from -0.09375 to 0.09375
- closing_standardize_scale: float32 [4096], replicated, may hold values from 0.7 to 2
- lexicon_projection: bfloat16 [4096, 65536], P(None, ('head', 'batch')), may hold values from -32 to 32
- proposed_tokens_list: int32 [64, 8], P('batch'), may hold values from 0 to 65535
- threshold_milli_nats: int32 [64, 8], P('batch'), may hold values from -22000 to -10001
Outputs:
- new_state: float32 [64, 64, 64, 64], P('batch', 'head')
- margin: float32 [64, 8], P('batch')
- accept: float32 [64, 8], P('batch')
The draws below stay inside these ranges and needn't reach their ends.
All inputs are finite; a program needn't handle non-finite values.
Results may differ from the reference program's by a relative error of at most 0.0017.
Values may be sent and summed in bfloat16 or wider, within the bound.
No kernel may reach another device: no remote copies, remote signals or barrier semaphores. Data moves between devices by JAX's collectives and lax.ppermute only.
A program may use at most 128 MiB of HBM per device.

```python
import math
import jax
import jax.numpy as jnp
from jax import lax

EMBED_DIM = 4096
ATTN_LANES = 64
SUBSPACE_SIZE = 64
VOCAB = 65536
DRAFT = 8
SEQS = 64
TOKENS = 512


def draw_closing_standardize_scale(key, part):
    return jax.random.uniform(key, (EMBED_DIM,), jnp.float32, 0.7, 1.4)


def draw_lexicon_projection(key, part):
    noise_key = jax.random.fold_in(key, 11)
    sign_key = jax.random.fold_in(key, 23)
    noise = jnp.clip(jax.random.normal(noise_key, (EMBED_DIM, VOCAB), jnp.float32) * 0.046875, -0.3, 0.3)
    signs = jax.random.randint(sign_key, (EMBED_DIM, 1), 0, 2).astype(jnp.float32) * 2.0 - 1.0
    rowpos = jax.lax.broadcasted_iota(jnp.int32, (EMBED_DIM, 1), 0)
    shifted = jnp.where(rowpos < 8, 32.0 * signs, noise)
    return shifted.astype(jnp.bfloat16)


def place_ends(entries, key, low, top_value):
    longest = entries.shape.index(max(entries.shape))
    spots = []
    for shift in (0, 1):
        where = [jax.random.randint(jax.random.fold_in(key, axis), (), 0, length) for axis, length in enumerate(entries.shape)]
        where[longest] = (where[longest] + shift) % entries.shape[longest]
        spots.append(tuple(where))
    return entries.at[spots[0]].set(low).at[spots[1]].set(top_value)


def levels(stream_key, shape, cuts, smallest, top_value):
    gain = 1.0
    for dim, shards_of in cuts:
        heights = jax.random.uniform(jax.random.fold_in(jax.random.fold_in(stream_key, 6), dim), (shards_of,), jnp.float32, smallest / len(cuts), top_value / len(cuts))
        gain = gain * jnp.repeat(jnp.exp(heights), shape[dim] // shards_of).reshape((-1,) + (1,) * (len(shape) - 1 - dim))
    return gain


def normal_values(rng, dims, scale, bound, shards=(), dtype=jnp.bfloat16):
    drawn = scale * jax.random.normal(rng, dims, jnp.float32)
    if shards:
        drawn = drawn * levels(rng, dims, shards, -0.22, 0.18)
    return jnp.clip(drawn, -bound, bound).astype(dtype)


def setup_inputs(seed: int = 0) -> dict:
    arg_keys = jax.random.split(jax.random.key(seed), 16)
    incoming_hidden_stream = normal_values(arg_keys[0], (TOKENS, EMBED_DIM), 1.0, 6.0, ((0, 4),))
    reception_projection = normal_values(arg_keys[1], (EMBED_DIM, EMBED_DIM), EMBED_DIM ** -0.5, 0.09375, ((1, 8),))
    address_projection = normal_values(arg_keys[2], (EMBED_DIM, EMBED_DIM), EMBED_DIM ** -0.5, 0.09375, ((1, 8),))
    payload_projection = normal_values(arg_keys[3], (EMBED_DIM, EMBED_DIM), EMBED_DIM ** -0.5, 0.09375, ((1, 8),))
    sigmoid_filter_matrix = normal_values(arg_keys[4], (EMBED_DIM, EMBED_DIM), EMBED_DIM ** -0.5, 0.09375, ((1, 8),))
    forgetting_speed = jnp.clip(jnp.exp(math.log(1.5) - 5.0106353 * jax.random.uniform(arg_keys[5], (TOKENS, EMBED_DIM), jnp.float32) ** levels(arg_keys[5], (TOKENS, EMBED_DIM), ((0, 4), (1, 8)), -0.2, 0.2)), 0.01, 1.5)
    adaptation_step_size = jnp.clip(1.0 * jax.random.uniform(arg_keys[6], (TOKENS, EMBED_DIM), jnp.float32) ** levels(arg_keys[6], (TOKENS, EMBED_DIM), ((0, 4), (1, 8)), -0.2, 0.2), 0.0, 1.0)
    diagonal_boost = normal_values(arg_keys[7], (EMBED_DIM,), 0.1, 0.6, ((0, 8),), jnp.float32)
    subspace_standardize_scale = jnp.clip(0.5 + 1.5 * jax.random.uniform(arg_keys[8], (EMBED_DIM,), jnp.float32) ** levels(arg_keys[8], (EMBED_DIM,), ((0, 8),), -0.2, 0.2), 0.5, 2.0)
    recurrent_memory_matrix = normal_values(arg_keys[9], (SEQS, ATTN_LANES, SUBSPACE_SIZE, SUBSPACE_SIZE), 1.0, 6.0, ((0, 4), (1, 8)), jnp.float32)
    emission_projection = normal_values(arg_keys[10], (EMBED_DIM, EMBED_DIM), EMBED_DIM ** -0.5, 0.09375, ((0, 8),))
    closing_standardize_scale = draw_closing_standardize_scale(jax.random.fold_in(arg_keys[15], 71), 0)
    lexicon_projection = draw_lexicon_projection(jax.random.fold_in(arg_keys[15], 71), 0)
    proposed_tokens_list = place_ends(jax.random.randint(arg_keys[13], (SEQS, DRAFT), 0, VOCAB), jax.random.fold_in(arg_keys[13], 1), 0, VOCAB - 1).astype(jnp.int32)
    threshold_milli_nats = place_ends(jax.random.randint(arg_keys[14], (SEQS, DRAFT), -22000, -10000), jax.random.fold_in(arg_keys[14], 1), -22000, (-10000) - 1).astype(jnp.int32)
    return {"incoming_hidden_stream": incoming_hidden_stream, "reception_projection": reception_projection, "address_projection": address_projection, "payload_projection": payload_projection, "sigmoid_filter_matrix": sigmoid_filter_matrix, "forgetting_speed": forgetting_speed, "adaptation_step_size": adaptation_step_size, "diagonal_boost": diagonal_boost, "subspace_standardize_scale": subspace_standardize_scale, "recurrent_memory_matrix": recurrent_memory_matrix, "emission_projection": emission_projection, "closing_standardize_scale": closing_standardize_scale, "lexicon_projection": lexicon_projection, "proposed_tokens_list": proposed_tokens_list, "threshold_milli_nats": threshold_milli_nats}


def advance(start, reception_vectors, address_vectors, payload_vectors, decay, rate):
    unit = address_vectors * lax.rsqrt(lax.optimization_barrier(jnp.mean(address_vectors * address_vectors, -1, keepdims=True)) + 1e-06) / math.sqrt(address_vectors.shape[-1])
    inputs = tuple((jnp.moveaxis(item, 1, 0) for item in (reception_vectors, address_vectors, payload_vectors, decay, unit, rate)))

    def step(current, pieces):
        recept_now, keys_now, values_now, decay_now, unit_now, rate_now = pieces
        recall = jnp.einsum('bhij,bhj->bhi', current, unit_now, precision=lax.Precision.HIGHEST)
        current = current * decay_now[:, :, None, :] - recall[:, :, :, None] * (unit_now * rate_now)[:, :, None, :] + values_now[:, :, :, None] * keys_now[:, :, None, :]
        output = jnp.einsum('bhij,bhj->bhi', current, recept_now, precision=lax.Precision.HIGHEST)
        return (current, output)
    final, outputs = lax.scan(step, start, inputs)
    return (final, jnp.moveaxis(outputs, 0, 1))

def reference(incoming_hidden_stream, reception_projection, address_projection, payload_projection, sigmoid_filter_matrix, forgetting_speed, adaptation_step_size, diagonal_boost, subspace_standardize_scale, recurrent_memory_matrix, emission_projection, closing_standardize_scale, lexicon_projection, proposed_tokens_list, threshold_milli_nats):
    shape4 = (SEQS, DRAFT, ATTN_LANES, SUBSPACE_SIZE)
    reception_vectors = jnp.dot(incoming_hidden_stream, reception_projection, preferred_element_type=jnp.float32).reshape(shape4)
    address_vectors = jnp.dot(incoming_hidden_stream, address_projection, preferred_element_type=jnp.float32).reshape(shape4)
    payload_vectors = jnp.dot(incoming_hidden_stream, payload_projection, preferred_element_type=jnp.float32).reshape(shape4)
    gate = jnp.dot(incoming_hidden_stream, sigmoid_filter_matrix, preferred_element_type=jnp.float32)
    decay = jnp.exp(-forgetting_speed).reshape(shape4)
    rate = adaptation_step_size.reshape(shape4)
    new_state, wkv = advance(recurrent_memory_matrix, reception_vectors, address_vectors, payload_vectors, decay, rate)
    center = wkv - lax.optimization_barrier(jnp.mean(wkv, -1, keepdims=True))
    interpolated_embedding = center * lax.rsqrt(lax.optimization_barrier(jnp.mean(center * center, -1, keepdims=True)) + 1e-05) * subspace_standardize_scale.reshape(ATTN_LANES, SUBSPACE_SIZE)
    interpolated_embedding = interpolated_embedding + lax.optimization_barrier(jnp.sum(reception_vectors * address_vectors * diagonal_boost.reshape(ATTN_LANES, SUBSPACE_SIZE), -1, keepdims=True)) * payload_vectors
    gated = (interpolated_embedding.reshape(TOKENS, EMBED_DIM) * jax.nn.sigmoid(gate)).astype(jnp.bfloat16)
    residual = incoming_hidden_stream.astype(jnp.float32) + jnp.dot(gated, emission_projection, preferred_element_type=jnp.float32)
    centered = residual - lax.optimization_barrier(jnp.mean(residual, -1, keepdims=True))
    normed = (centered * lax.rsqrt(lax.optimization_barrier(jnp.mean(centered * centered, -1, keepdims=True)) + 1e-05) * closing_standardize_scale).astype(jnp.bfloat16)
    logits = jnp.dot(normed, lexicon_projection, preferred_element_type=jnp.float32)
    peak = lax.optimization_barrier(jnp.max(logits, -1))
    total = lax.optimization_barrier(jnp.sum(jnp.exp(logits - peak[:, None]), -1))
    target = jnp.take_along_axis(logits, proposed_tokens_list.reshape(TOKENS, 1).astype(jnp.int32), 1)[:, 0]
    logprob = target - (peak + jnp.log(total))
    margin = logprob.reshape(SEQS, DRAFT) - threshold_milli_nats.astype(jnp.float32) / 1000.0
    accept = jnp.cumprod(jax.nn.sigmoid(margin * 0.5), axis=1)
    return (new_state, margin, accept)
```

```python
import functools
import math

import jax
import jax.numpy as jnp
from jax import lax
from jax.experimental import pallas as pl
from jax.experimental.pallas import tpu as pltpu
from jax.sharding import PartitionSpec as P

F32 = jnp.float32
BF16 = jnp.bfloat16
LANES = 128
ROW_PAD = 8
VMEM = pl.BlockSpec(memory_space=pltpu.VMEM)
ANY = pl.BlockSpec(memory_space=pl.ANY)
VMEM_LIMIT = 64 * 1024 * 1024 - 65536


def time_mix_body(
    x_hbm, wr_hbm, wk_hbm, wv_hbm, wg_hbm, speed_hbm, rate_hbm, boost_ref, scale_ref, state_hbm, emission_hbm,
    out_ref, state_ref,
    x, wr, wk, wv, wg, emission, speed, rate, raw, state, recept, keys, values, gate, mixed,
    recept_t, keys_t, values_t, unit_t, step_t, decay_t, wkv_t, sems,
    *, seqs, draft, heads, sub,
):
    tiles, tokens, _ = speed.shape
    channels = tiles * LANES
    pitch = heads * sub + ROW_PAD
    per_tile = LANES // sub
    half = tiles * seqs
    pairs = per_tile * half

    plain = [(x_hbm, x), (wk_hbm, wk), (wr_hbm, wr), (wv_hbm, wv), (wg_hbm, wg), (emission_hbm, emission)]
    for src, dst in ((speed_hbm, speed), (rate_hbm, rate)):
        plain += [(src.at[:, pl.ds(m * LANES, LANES)], dst.at[m]) for m in range(tiles)]
    copies = [pltpu.make_async_copy(src, dst, sems.at[n]) for n, (src, dst) in enumerate(plain)]
    state_copies = [
        pltpu.make_async_copy(state_hbm.at[b], raw.at[b], sems.at[len(plain) + b])
        for b in range(seqs)
    ]
    copies[0].start()
    for c in state_copies:
        c.start()
    for c in copies[1:]:
        c.start()

    for b in range(seqs):
        state_copies[b].wait()
        state[pl.ds(b * pitch, heads * sub), pl.ds(0, sub)] = raw[b]

    def turn_in(i, carry):
        rows = [
            state[pl.ds((m * per_tile + s) * sub + i, seqs, stride=pitch), :]
            for s in range(per_tile)
            for m in range(tiles)
        ]
        state_ref[i] = jnp.concatenate(rows, axis=0).T[:sub]
        return carry

    lax.fori_loop(0, sub, turn_in, 0, unroll=4)

    def project(n, w, dst):
        copies[n].wait()
        width = min(256, channels)
        for c in range(0, channels, width):
            found = jnp.dot(x[...], w[:, c : c + width], preferred_element_type=F32)
            for q in range(0, width, LANES):
                dst[(c + q) // LANES] = found[:, q : q + LANES]

    copies[0].wait()
    project(1, wk, keys)
    project(2, wr, recept)
    project(3, wv, values)
    for c in copies[6:]:
        c.wait()

    def rows_of(ref, t):
        return jnp.concatenate(
            [ref[m, pl.ds(t, seqs, stride=draft), :] for m in range(tiles)], axis=0
        )

    def turn(first, second):
        z = jnp.concatenate([first, second], axis=0).T
        return tuple(
            jnp.concatenate([z[s * sub : (s + 1) * sub, k * half : (k + 1) * half] for s in range(per_tile)], axis=1)
            for k in range(2)
        )

    def spread(ref):
        return jnp.concatenate(
            [jnp.broadcast_to(ref[:, m * LANES : (m + 1) * LANES], (seqs, LANES)) for m in range(tiles)], axis=0
        )

    boost, scale = turn(spread(boost_ref), spread(scale_ref))

    def prepare(t, carry):
        r, k = turn(rows_of(recept, t), rows_of(keys, t))
        v, f = turn(rows_of(values, t), rows_of(speed, t))
        a, _ = turn(rows_of(rate, t), rows_of(rate, t))
        unit = k * lax.rsqrt(jnp.mean(k * k, axis=0, keepdims=True) + 1e-06) / math.sqrt(sub)
        recept_t[t] = r
        keys_t[t] = k
        values_t[t] = v
        unit_t[t] = unit
        step_t[t] = unit * a
        decay_t[t] = jnp.exp(-f)
        return carry

    lax.fori_loop(0, draft, prepare, 0)

    block = 2

    def advance(n, carry):
        i = n * block
        s = [state_ref[i + q] for q in range(block)]
        for t in range(draft):
            unit, step, k, decay, r = unit_t[t], step_t[t], keys_t[t], decay_t[t], recept_t[t]
            for q in range(block):
                recall = jnp.sum(s[q] * unit, axis=0, keepdims=True)
                s[q] = s[q] * decay - recall * step + values_t[t, pl.ds(i + q, 1), :] * k
                wkv_t[t, pl.ds(i + q, 1), :] = jnp.sum(s[q] * r, axis=0, keepdims=True)
        for q in range(block):
            state_ref[i + q] = s[q]
        return carry

    lax.fori_loop(0, sub // block, advance, 0)

    project(4, wg, gate)

    def normed(t):
        o = wkv_t[t]
        center = o - jnp.mean(o, axis=0, keepdims=True)
        o = center * lax.rsqrt(jnp.mean(center * center, axis=0, keepdims=True) + 1e-05) * scale
        bonus = jnp.sum(recept_t[t] * keys_t[t] * boost, axis=0, keepdims=True)
        return o + bonus * values_t[t]

    def finish(n, carry):
        t = n * 2
        both = (normed(t), normed(t + 1))
        z = jnp.concatenate(
            [jnp.concatenate([o[:, s * half : (s + 1) * half] for o in both], axis=1) for s in range(per_tile)], axis=0
        ).T
        for k in range(2):
            for m in range(tiles):
                row = k * half + m * seqs
                mixed[m, pl.ds(t + k, seqs, stride=draft), :] = z[row : row + seqs, :]
        return carry

    lax.fori_loop(0, draft // 2, finish, 0)

    gated = jnp.concatenate([(mixed[m] * jax.nn.sigmoid(gate[m])).astype(BF16) for m in range(tiles)], axis=1)
    copies[5].wait()
    width = min(512, emission.shape[1])
    for c in range(0, emission.shape[1], width):
        out_ref[:, c : c + width] = jnp.dot(gated, emission[:, c : c + width], preferred_element_type=F32).astype(BF16)


def time_mix(x, wr, wk, wv, wg, speed, rate, boost, scale, state, emission):
    seqs, heads, sub, _ = state.shape
    tokens, channels = speed.shape
    draft = tokens // seqs
    width = x.shape[1]
    pairs = seqs * heads
    weight = pltpu.VMEM(wr.shape, BF16)
    flat = pltpu.VMEM((channels // LANES, tokens, LANES), F32)
    turned = pltpu.VMEM((draft, sub, pairs), F32)
    body = functools.partial(time_mix_body, seqs=seqs, draft=draft, heads=heads, sub=sub)
    flops = 2 * tokens * width * channels * 5
    return pl.pallas_call(
        body,
        in_specs=[ANY] * 7 + [VMEM] * 2 + [ANY] * 2,
        out_specs=[VMEM, VMEM],
        out_shape=[
            jax.ShapeDtypeStruct((tokens, width), BF16),
            jax.ShapeDtypeStruct((sub, sub, pairs), F32),
        ],
        scratch_shapes=[pltpu.VMEM(x.shape, BF16)]
        + [weight] * 4
        + [pltpu.VMEM(emission.shape, BF16), flat, flat, pltpu.VMEM((seqs, heads * sub, sub), F32), pltpu.VMEM((seqs * (heads * sub + ROW_PAD), LANES), F32)]
        + [flat] * 5
        + [turned] * 7
        + [pltpu.SemaphoreType.DMA((6 + 2 * (channels // LANES) + seqs,))],
        compiler_params=pltpu.CompilerParams(vmem_limit_bytes=VMEM_LIMIT),
        cost_estimate=pl.CostEstimate(flops=flops, bytes_accessed=32 << 20, transcendentals=0),
        name="time_mix",
    )(
        x, wr, wk, wv, wg, speed, rate, boost.reshape(1, -1), scale.reshape(1, -1),
        state.reshape(seqs, heads * sub, sub), emission,
    )


def turn_out_body(turned, out_ref, wide, *, seqs, heads, sub):
    pitch = heads * sub + ROW_PAD
    per_tile = LANES // sub
    tiles = heads // per_tile

    def one(i, carry):
        z = jnp.concatenate([turned[i], turned[i]], axis=0).T
        for s in range(per_tile):
            for m in range(tiles):
                row = (s * tiles + m) * seqs
                wide[pl.ds((m * per_tile + s) * sub + i, seqs, stride=pitch), :] = z[row : row + seqs, :]
        return carry

    lax.fori_loop(0, sub, one, 0, unroll=4)
    for b in range(seqs):
        out_ref[b] = wide[pl.ds(b * pitch, heads * sub), pl.ds(0, sub)]


def turn_out(turned, shape):
    seqs, heads, sub, _ = shape
    out = pl.pallas_call(
        functools.partial(turn_out_body, seqs=seqs, heads=heads, sub=sub),
        in_specs=[VMEM],
        out_specs=VMEM,
        out_shape=jax.ShapeDtypeStruct((seqs, heads * sub, sub), F32),
        scratch_shapes=[pltpu.VMEM((seqs * (heads * sub + ROW_PAD), LANES), F32)],
        compiler_params=pltpu.CompilerParams(vmem_limit_bytes=VMEM_LIMIT),
        cost_estimate=pl.CostEstimate(flops=1 << 30, bytes_accessed=8 << 20, transcendentals=0),
        name="turn_out",
    )(turned)
    return out.reshape(shape)


def settle_body(parts_ref, x_hbm, scale_ref, ids_ref, out_ref, own, sem, *, chunk):
    me = lax.axis_index("head")
    width = x_hbm.shape[1]
    copy = pltpu.make_async_copy(x_hbm.at[pl.ds(pl.multiple_of(me * chunk, chunk), chunk), :], own, sem)
    copy.start()
    total = parts_ref[0:chunk, :].astype(F32)
    for k in range(1, parts_ref.shape[0] // chunk):
        total = total + parts_ref[k * chunk : (k + 1) * chunk, :].astype(F32)
    copy.wait()
    residual = own[...].astype(F32) + total
    centered = residual - jnp.mean(residual, axis=-1, keepdims=True)
    spread = lax.rsqrt(jnp.mean(centered * centered, axis=-1, keepdims=True) + 1e-05)
    out_ref[:, :width] = (centered * spread * scale_ref[...]).astype(BF16)
    draft, seqs = ids_ref.shape
    lane = lax.broadcasted_iota(jnp.int32, (draft, seqs), 1)
    first = me * (chunk // draft)
    ids = jnp.concatenate(
        [
            jnp.sum(jnp.where(lane == first + k, ids_ref[...], 0), axis=1, keepdims=True)
            for k in range(chunk // draft)
        ],
        axis=0,
    )
    lane = lax.broadcasted_iota(jnp.int32, (chunk, LANES), 1)
    digits = jnp.where(lane < 3, (ids >> (8 * jnp.minimum(lane, 2))) & 255, 0)
    out_ref[:, width:] = digits.astype(F32).astype(BF16)


def settle(parts, x, scale, ids, chunk):
    width = x.shape[1]
    return pl.pallas_call(
        functools.partial(settle_body, chunk=chunk),
        in_specs=[VMEM, ANY, VMEM, VMEM],
        out_specs=VMEM,
        out_shape=jax.ShapeDtypeStruct((chunk, width + LANES), BF16),
        scratch_shapes=[pltpu.VMEM((chunk, width), BF16), pltpu.SemaphoreType.DMA],
        compiler_params=pltpu.CompilerParams(vmem_limit_bytes=VMEM_LIMIT),
        name="settle",
    )(parts, x, scale.reshape(1, -1), ids.T)


def score_body(*refs, counts, spots, carried, last, grid_n, shape):
    heads, batches, chunk = shape
    n_in = len(counts)
    pieces = refs[:n_in]
    lexicon = refs[n_in]
    pos = n_in + 1
    before = refs[pos : pos + 3] if carried else ()
    pos += len(before)
    if last:
        out_ref, rows_ref, wanted, top, total, target, top_all, total_all, target_all = refs[pos:]
    else:
        top, total, target, rows_ref, wanted = refs[pos:]
    step = pl.program_id(0)
    tile = lexicon.shape[1]
    width = lexicon.shape[0]

    @pl.when(step == 0)
    def _():
        me = lax.axis_index("head") * batches + lax.axis_index("batch")
        row = 0
        for piece, count in zip(pieces, counts):
            rows_ref[row : row + count, :] = piece[:, :width]
            digits = piece[:, width:].astype(F32)
            ids = digits[:, 0:1] + 256.0 * digits[:, 1:2] + 65536.0 * digits[:, 2:3]
            ids = ids.astype(jnp.int32) - me * (tile * grid_n)
            lane = lax.broadcasted_iota(jnp.int32, (count, LANES), 1)
            wanted[row : row + count, :] = ids - lane
            row += count
        top[...] = jnp.full(top.shape, -jnp.inf, F32)
        total[...] = jnp.zeros(total.shape, F32)
        target[...] = jnp.zeros(target.shape, F32)

    logits = jnp.dot(rows_ref[...], lexicon[...], preferred_element_type=F32)
    parts = [logits[:, q : q + LANES] for q in range(0, tile, LANES)]
    high = top[...]
    for p in parts:
        high = jnp.maximum(high, p)
    grown = total[...] * jnp.exp(top[...] - high)
    found = target[...]
    goal = wanted[...] - step * tile
    for q, p in enumerate(parts):
        grown = grown + jnp.exp(p - high)
        found = found + jnp.where(goal == q * LANES, p, 0.0)
    top[...] = high
    total[...] = grown
    target[...] = found

    if last:

        @pl.when(step == grid_n - 1)
        def _():
            sources = [(top, total, target, spots[-1])]
            if carried:
                sources.append((*before, spots[0]))
            for t, s, g, where_to in sources:
                for k, spot in enumerate(where_to):
                    head, batch = spot()
                    to = pl.ds(pl.multiple_of((batch * heads + head) * chunk, chunk), chunk)
                    top_all[to, :] = t[k * chunk : (k + 1) * chunk, :]
                    total_all[to, :] = s[k * chunk : (k + 1) * chunk, :]
                    target_all[to, :] = g[k * chunk : (k + 1) * chunk, :]
            span = heads * chunk
            for b in range(batches):
                at = slice(b * span, (b + 1) * span)
                t = top_all[at, :].T
                peak = jnp.max(t, axis=0, keepdims=True)
                s = jnp.sum(total_all[at, :].T * jnp.exp(t - peak), axis=0, keepdims=True)
                level = peak + jnp.log(s)
                goal = jnp.sum(target_all[at, :].T, axis=0, keepdims=True)
                row = jnp.concatenate([level, goal], axis=1)
                for h in range(heads):
                    out_ref[h * batches + b : h * batches + b + 1, :] = row


def score(pieces, lexicon, spots, shape, before=None, last=True, tile=512):
    heads, batches, chunk = shape
    width, columns = lexicon.shape
    tile = min(tile, columns)
    counts = tuple(p.shape[0] for p in pieces)
    rows = sum(counts)
    carried = before is not None
    grid_n = columns // tile
    stat = (rows, LANES)
    whole = lambda a: pl.BlockSpec(a.shape, lambda n: (0, 0))
    in_specs = [whole(p) for p in pieces] + [pl.BlockSpec((width, tile), lambda n: (0, n))]
    operands = list(pieces) + [lexicon]
    if carried:
        in_specs += [whole(a) for a in before]
        operands += list(before)
    everyone = heads * batches * chunk
    held = [pltpu.VMEM((rows, width), BF16), pltpu.VMEM(stat, jnp.int32)]
    if last:
        out_shape = jax.ShapeDtypeStruct((heads * batches, 2 * heads * chunk), F32)
        out_specs = pl.BlockSpec(out_shape.shape, lambda n: (0, 0))
        scratch = held + [pltpu.VMEM(stat, F32)] * 3 + [pltpu.VMEM((everyone, LANES), F32)] * 3
    else:
        out_shape = [jax.ShapeDtypeStruct(stat, F32)] * 3
        out_specs = [pl.BlockSpec(stat, lambda n: (0, 0))] * 3
        scratch = held
    return pl.pallas_call(
        functools.partial(
            score_body, counts=counts, spots=spots, carried=carried, last=last, grid_n=grid_n, shape=shape
        ),
        grid=(grid_n,),
        in_specs=in_specs,
        out_specs=out_specs,
        out_shape=out_shape,
        scratch_shapes=scratch,
        compiler_params=pltpu.CompilerParams(vmem_limit_bytes=VMEM_LIMIT),
        cost_estimate=pl.CostEstimate(
            flops=2 * rows * width * columns, bytes_accessed=2 * width * columns, transcendentals=rows * columns
        ),
        name="score",
    )(*operands)


def verdict_body(stats_ref, threshold_ref, margin_ref, accept_ref):
    draft, seqs = threshold_ref.shape
    tokens = draft * seqs
    level, goal = stats_ref[:, :tokens], stats_ref[:, tokens:]
    peak = jnp.max(level, axis=0, keepdims=True)
    total = jnp.sum(jnp.exp(level - peak), axis=0, keepdims=True)
    logprob = jnp.sum(goal, axis=0, keepdims=True) - (peak + jnp.log(total))
    place = lax.broadcasted_iota(jnp.int32, (draft, tokens), 1) % draft
    mine = lax.broadcasted_iota(jnp.int32, (draft, tokens), 0)
    laid = jnp.where(place == mine, jnp.broadcast_to(logprob, (draft, tokens)), 0.0)
    seq = lax.broadcasted_iota(jnp.int32, (tokens, seqs), 0) // draft
    pick = jnp.where(seq == lax.broadcasted_iota(jnp.int32, (tokens, seqs), 1), 1.0, 0.0)
    laid = jnp.dot(laid, pick, precision=lax.Precision.HIGHEST, preferred_element_type=F32)
    margin = laid - threshold_ref[...].astype(F32) / 1000.0
    margin_ref[...] = margin
    chance = jax.nn.sigmoid(margin * 0.5)
    so_far = chance[0:1, :]
    accept_ref[0:1, :] = so_far
    for t in range(1, draft):
        so_far = so_far * chance[t : t + 1, :]
        accept_ref[t : t + 1, :] = so_far


def verdict(stats, threshold):
    seqs, draft = threshold.shape
    out = jax.ShapeDtypeStruct((draft, seqs), F32)
    margin, accept = pl.pallas_call(
        verdict_body,
        in_specs=[VMEM, VMEM],
        out_specs=[VMEM, VMEM],
        out_shape=[out, out],
        name="verdict",
    )(stats, threshold.T)
    return margin.T, accept.T


BOTH = ("head", "batch")


def gather_tokens(own, nz, ny, nx, nc):
    place = lambda z, y, x, c: ((z * ny + y) * nx + x) * nc + c

    def shift(data, move):
        pairs = []
        for z in range(nz):
            for y in range(ny):
                for x in range(nx):
                    for c in range(nc):
                        dz, dy, dx, dc = move(c)
                        to = place((z + dz) % nz, (y + dy) % ny, (x + dx) % nx, (c + dc) % nc)
                        pairs.append((place(z, y, x, c), to))
        return lax.ppermute(data, BOTH, pairs)

    def moved(spots, move):
        return [
            lambda c, s=s: tuple((a + b) for a, b in zip(s(c), move(c)))
            for s in spots
        ]

    first = [own] + [shift(own, lambda c, k=k: (k, 0, 0, 0)) for k in range(1, nz)]
    spots = [lambda c, k=k: (k, 0, 0, 0) for k in range(nz)]
    column = jnp.concatenate(first, axis=0)
    return column, spots, shift, moved


def shards(
    incoming_hidden_stream,
    reception_projection,
    address_projection,
    payload_projection,
    sigmoid_filter_matrix,
    forgetting_speed,
    adaptation_step_size,
    diagonal_boost,
    subspace_standardize_scale,
    recurrent_memory_matrix,
    emission_projection,
    closing_standardize_scale,
    lexicon_projection,
    proposed_tokens_list,
    threshold_milli_nats,
):
    heads, batches = lax.axis_size("head"), lax.axis_size("batch")
    tokens = incoming_hidden_stream.shape[0]
    chunk = tokens // heads
    partial_out, turned = time_mix(
        incoming_hidden_stream,
        reception_projection,
        address_projection,
        payload_projection,
        sigmoid_filter_matrix,
        forgetting_speed,
        adaptation_step_size,
        diagonal_boost,
        subspace_standardize_scale,
        recurrent_memory_matrix,
        emission_projection,
    )
    parts = lax.all_to_all(partial_out, "head", 0, 0, tiled=True)
    own = settle(parts, incoming_hidden_stream, closing_standardize_scale, proposed_tokens_list, chunk)

    nc = 2 if batches % 2 == 0 else 1
    nx = batches // nc
    nz = 4 if heads % 4 == 0 else heads
    ny = heads // nz
    column, spots, shift, moved = gather_tokens(own, nz, ny, nx, nc)
    pieces = [(column, spots)]
    along_y = lambda k: (lambda c: (0, k, 0, 0))
    along_x = lambda k: (lambda c: (0, 0, k, 0))
    if nc == 2 and nx == ny:
        one = lambda k: (lambda c: (0, k, 0, 0) if c == 0 else (0, 0, k, 0))
        two = lambda k: (lambda c: (0, 0, k, 0) if c == 0 else (0, k, 0, 0))
        n_one = n_two = nx
    else:
        one, two, n_one, n_two = along_y, along_x, ny, nx
    seconds = [(shift(column, one(k)), moved(spots, one(k))) for k in range(1, n_one)]
    thirds = [(shift(column, two(k)), moved(spots, two(k))) for k in range(1, n_two)]
    fourths = [(shift(d, two(k)), moved(s, two(k))) for d, s in seconds for k in range(1, n_two)]
    early = [pieces[0]] + seconds + thirds
    swap = lambda c: (0, 0, 0, 1)
    across = lambda group: [(shift(d, swap), [lambda c, t=t: tuple(a + b for a, b in zip(t(1 - c), (0, 0, 0, 1))) for t in s]) for d, s in group] if nc == 2 else []
    early = early + across(early)
    late = fourths + across(fourths)

    def spot_of(s):
        def find():
            head, batch = lax.axis_index("head"), lax.axis_index("batch")
            z, y, x, c = head // ny, head % ny, batch // nc, batch % nc
            by_core = [s(k) for k in range(nc)]
            offs = [by_core[0][d] if nc == 1 else jnp.where(c == 0, by_core[0][d], by_core[1][d]) for d in range(4)]
            sz, sy, sx, sc = ((p - o + n * 4) % n for p, o, n in zip((z, y, x, c), offs, (nz, ny, nx, nc)))
            return sz * ny + sy, sx * nc + sc

        return find

    shape = (heads, batches, chunk)
    early_spots = [spot_of(t) for _, s in early for t in s]
    late_spots = [spot_of(t) for _, s in late for t in s]
    if late:
        before = score([d for d, _ in early], lexicon_projection, None, shape, last=False)
        stats = score([d for d, _ in late], lexicon_projection, (early_spots, late_spots), shape, before=before)
    else:
        stats = score([d for d, _ in early], lexicon_projection, (early_spots,), shape)
    new_state = turn_out(turned, recurrent_memory_matrix.shape)
    stats = lax.all_to_all(stats, BOTH, 0, 0, tiled=True)
    margin, accept = verdict(stats, threshold_milli_nats)
    return (new_state, margin, accept)


def solution(mesh):
    in_specs = (
        P("batch", None),
        P(None, "head"),
        P(None, "head"),
        P(None, "head"),
        P(None, "head"),
        P("batch", "head"),
        P("batch", "head"),
        P("head"),
        P("head"),
        P("batch", "head", None, None),
        P("head", None),
        P(),
        P(None, ("head", "batch")),
        P("batch", None),
        P("batch", None),
    )
    out_specs = (P("batch", "head", None, None), P("batch", None), P("batch", None))
    return jax.shard_map(shards, mesh=mesh, in_specs=in_specs, out_specs=out_specs, check_vma=False)
```
